32 devices in a mesh: groups: 2 (over x), cent: 16 (over z, y, core).
Axes of the slice: x: 2, y: 2, z: 4, core: 2. Of those that a mesh axis runs over, the one named last changes fastest.
Arguments:
- points: bfloat16 [1024, 768], P(('groups', 'cent')), parts along dimension 0, may hold values from -64 to 64, as said below
- centroids: bfloat16 [131072, 768], P(('groups', 'cent')), parts along dimension 0, may hold values from -1 to 1
- coarse_init: float32 [4096, 768], P(('groups', 'cent')), parts along dimension 0, may hold values from -2.4 to 2.4
- assign: int32 [131072], P(('groups', 'cent')), parts along dimension 0, may hold values from 0 to 2047, as said below
Outputs:
- level_one: bfloat16 [131072, 768], P(('groups', 'cent')), parts along dimension 0
- level_two: float32 [4096, 768], P(('groups', 'cent')), parts along dimension 0
The draws below stay inside these ranges and needn't reach their ends.
There are 2 independent parts, one for each index of `groups`. The reference program is written for one: setup_inputs(seed, part) draws one part's arguments, and reference() takes and returns one part's arrays. A program takes and returns all parts, laid end to end along the dimension named above; each array names one. Nothing has to cross between parts.
Inputs may be any that keep to these rules, and one draw needn't show every extreme that they name: `points`: entries normal (clipped at 8) or uniform within 1.7; on some draws a few rows are scaled multiples of a centroid that has a close twin, giving logits up to about 300. `assign`: among the 65536 // 16 level-1 centroids held by one index of cent, at most 512 have their level-2 centroid in any one block of 2048 // 16 consecutive level-2 centroids, and some block receives exactly 512.
All inputs are finite; a program needn't handle non-finite values.
Results may differ from the reference program's by a relative error of at most 0.0039.
Values may be sent and summed in bfloat16 or wider, within the bound.
A program may use at most 64 MiB of HBM per device.

```python
import math
import jax
import jax.numpy as jnp
from jax import lax

D = 768
K1 = 65536
K2 = 2048
PTS = 512
CAP = 512
N_CENT = 16


def pair_draw(key):
    key_pts, key_cen = jax.random.split(jax.random.fold_in(key, 7), 2)
    points = jnp.clip(jax.random.normal(key_pts, (PTS, D), jnp.float32), -8.0, 8.0)
    cents = jnp.clip(0.1 * jax.random.normal(key_cen, (K1, D), jnp.float32), -0.8, 0.8)
    return (points, cents)


def draw_points(key, part):
    return pair_draw(key)[0].astype(jnp.bfloat16)


def draw_centroids(key, part):
    return pair_draw(key)[1].astype(jnp.bfloat16)


def draw_assign(key, part):
    local = K1 // N_CENT
    own = K2 // N_CENT
    limit = CAP

    def one_block(block_key):
        key_perm, key_mix, key_inner = jax.random.split(block_key, 3)
        owners = jax.random.permutation(key_perm, N_CENT)
        dest = owners[jnp.arange(local, dtype=jnp.int32) // limit]
        dest = jax.random.permutation(key_mix, dest)
        inner = jax.random.randint(key_inner, (local,), 0, own, jnp.int32)
        return dest.astype(jnp.int32) * own + inner
    keys = jax.random.split(jax.random.fold_in(key, 11), N_CENT)
    return jax.vmap(one_block)(keys).reshape(K1).astype(jnp.int32)


def level_of(stream_key, extent, pieces, least, top_value):
    def one(axis_at, blocks):
        steps = jax.random.uniform(jax.random.fold_in(jax.random.fold_in(stream_key, 6), axis_at), (blocks,), jnp.float32, least / len(pieces), top_value / len(pieces))
        return jnp.repeat(jnp.exp(steps), extent[axis_at] // blocks).reshape((-1,) + (1,) * (len(extent) - axis_at - 1))

    gain = one(*pieces[0])
    for cut in pieces[1:]:
        gain = gain * one(*cut)
    return gain


def bell_draw(key, shape, spread, most, cuts=(), kind=jnp.bfloat16):
    drawn = jax.random.normal(key, shape, jnp.float32) * spread
    if len(cuts) > 0:
        drawn = level_of(key, shape, cuts, -0.22, 0.18) * drawn
    return jnp.clip(drawn, min=-most, max=most).astype(kind)


def setup_inputs(seed: int = 0, part: int = 0) -> dict:
    key_of = jax.random.split(jax.random.key(seed), 5)
    part_splits = jax.random.split(jax.random.fold_in(key_of[4], part), 5)
    points = draw_points(jax.random.fold_in(jax.random.fold_in(key_of[4], part), 71), part)
    centroids = draw_centroids(jax.random.fold_in(jax.random.fold_in(key_of[4], part), 71), part)
    coarse_init = bell_draw(part_splits[2], (K2, D), 0.3, 2.4, ((0, 16),), jnp.float32)
    assign = draw_assign(jax.random.fold_in(jax.random.fold_in(key_of[4], part), 71), part)
    return dict(points=points, centroids=centroids, coarse_init=coarse_init, assign=assign)


TEMP = 0.05
PRIOR_ONE = 0.02
PRIOR_TWO = 0.25

def reference(points, centroids, coarse_init, assign):
    scale = 1.0 / (TEMP * math.sqrt(D))
    width = min(4096, K1)
    cblocks = centroids.reshape(K1 // width, width, D)

    def logits_of(block):
        return jnp.dot(points, block.T, preferred_element_type=jnp.float32) * scale

    def top_step(carry, block):
        return (jnp.maximum(carry, lax.optimization_barrier(jnp.max(logits_of(block), axis=1))), None)
    peak, _ = lax.scan(top_step, jnp.full((PTS,), -jnp.inf, jnp.float32), cblocks)

    def sum_step(carry, block):
        return (carry + lax.optimization_barrier(jnp.sum(jnp.exp(logits_of(block) - peak[:, None]), axis=1)), None)
    total, _ = lax.scan(sum_step, jnp.zeros((PTS,), jnp.float32), cblocks)

    def update(block):
        resp = jnp.exp(logits_of(block) - peak[:, None]) / total[:, None]
        mass = lax.optimization_barrier(jnp.sum(resp, axis=0))
        weighted = jnp.dot(resp.astype(jnp.bfloat16).T, points, preferred_element_type=jnp.float32)
        fresh = (weighted + PRIOR_ONE * block.astype(jnp.float32)) / (mass[:, None] + PRIOR_ONE)
        return (fresh, mass)
    fresh, mass = lax.map(update, cblocks)
    fresh = fresh.reshape(K1, D)
    mass = mass.reshape(K1)
    level_one = fresh.astype(jnp.bfloat16)
    moved = (mass[:, None] * fresh).astype(jnp.bfloat16)
    wsum = jax.ops.segment_sum(moved.astype(jnp.float32), assign, K2)
    msum = jax.ops.segment_sum(mass, assign, K2)
    level_two = (wsum + PRIOR_TWO * coarse_init) / (msum[:, None] + PRIOR_TWO)
    return (level_one, level_two)
```

```python
import functools
import math

import jax
import jax.numpy as jnp
from jax import lax
from jax.experimental import pallas as pl
from jax.experimental.pallas import tpu as pltpu
from jax.sharding import PartitionSpec as P

TEMP = 0.05
PRIOR_ONE = 0.02
PRIOR_TWO = 0.25
LANES = 128
MESH = pl.DeviceIdType.MESH
ROWS_BY_ROWS = (((1,), (1,)), ((), ()))


def log2_scale(width):
    return math.log2(math.e) / (TEMP * math.sqrt(width))


def flip(z, e, lines):
    out, bit = 0, 1
    while bit < lines:
        out = out + bit * lax.rem(z // bit + e // bit, 2)
        bit *= 2
    return out


def stats_kernel(
    n, tile, pts_ref, cen_hbm, all_ref, lse_ref, cen, mine, theirs, cen_sem, line_sem, pair_sem, core_sem, sems
):
    group, me = lax.axis_index("groups"), lax.axis_index("cent")
    rows, width = pts_ref.shape
    part = rows // 2
    count = n * part
    lines = n // 4
    line, pair, core = me // 4, lax.rem(me // 2, 2), lax.rem(me, 2)
    tiles = cen.shape[0] // tile
    c2 = log2_scale(width)

    def fetch(t):
        part_of = pl.ds(t * tile, tile)
        return pltpu.make_async_copy(cen_hbm.at[part_of], cen.at[part_of], cen_sem.at[t])

    for t in range(tiles):
        fetch(t).start()

    barrier = pltpu.get_barrier_semaphore()

    @pl.loop(1, n)
    def _(off):
        peer = lax.rem(me + off, n)
        pl.semaphore_signal(barrier, inc=1, device_id=(group, peer), device_id_type=MESH)

    pl.semaphore_wait(barrier, n - 1)

    def slot(h, z, y, c):
        return pl.ds(pl.multiple_of(h * count + (z * 4 + y * 2 + c) * part, part), part)

    def send(src, where, sem, z, y, c):
        return pltpu.make_async_remote_copy(
            src_ref=src,
            dst_ref=all_ref.at[where],
            send_sem=sems.at[0],
            recv_sem=sem,
            device_id=(group, z * 4 + y * 2 + c),
            device_id_type=MESH,
        )

    def along(h, e, src, where):
        z = flip(line, e, lines)
        return send(src, where, line_sem.at[h, e], z, pair, core)

    def across(h, e, src, where):
        return send(src, where, pair_sem.at[h, e], line, 1 - pair, core)

    def over(h, src, where):
        return send(src, where, core_sem.at[h], line, pair, 1 - core)

    def relay_line(h):
        for e in range(1, lines):
            where = slot(h, flip(line, e, lines), pair, core)
            got = all_ref.at[where]
            along(h, e, got, where).wait_recv()
            across(h, e, got, where).start()
            over(h, got, where).start()

    def relay_pair(h):
        for e in range(lines):
            where = slot(h, flip(line, e, lines), 1 - pair, core)
            got = all_ref.at[where]
            across(h, e, got, where).wait_recv()
            over(h, got, where).start()

    def gathered(h):
        whole = all_ref.at[pl.ds(0, 2 * lines * part)]
        pltpu.make_async_copy(whole, whole, core_sem.at[h]).wait()

    for h in range(2):
        own = pts_ref.at[pl.ds(h * part, part)]
        where = slot(h, line, pair, core)
        for e in range(lines - 1, 0, -1):
            along(h, e, own, where).start()
        across(h, 0, own, where).start()
        over(h, own, where).start()
        all_ref[where, :] = pts_ref[pl.ds(h * part, part), :]

    def stats(h, first, last, carry):
        def step(t, carry):
            peak, total = carry
            if h == 0:
                fetch(t).wait()
            block = cen[pl.ds(pl.multiple_of(t * tile, tile), tile), :]
            pts = all_ref[pl.ds(h * count, count), :]
            logits = (
                lax.dot_general(block, pts, ROWS_BY_ROWS, preferred_element_type=jnp.float32) * c2
            )
            higher = jnp.maximum(peak, jnp.max(logits, axis=0, keepdims=True))
            total = total * jnp.exp2(peak - higher) + jnp.sum(
                jnp.exp2(logits - higher), axis=0, keepdims=True
            )
            return higher, total

        return lax.fori_loop(first, last, step, carry)

    def share(h, off):
        return pltpu.make_async_remote_copy(
            src_ref=mine.at[h],
            dst_ref=theirs.at[h, off - 1],
            send_sem=sems.at[1],
            recv_sem=sems.at[2 + h],
            device_id=(group, lax.rem(me + off, n)),
            device_id_type=MESH,
        )

    def publish(h, carry):
        peak, total = carry
        mine[h, 0:1, :] = peak
        mine[h, 1:2, :] = total

        @pl.loop(1, n)
        def _(off):
            share(h, off).start()

    def merge(h, carry):
        peak, total = carry
        got = theirs.at[h]
        pltpu.make_async_copy(got, got, sems.at[2 + h]).wait()
        both = theirs[h]
        top = jnp.maximum(peak, jnp.max(both[:, 0:1, :], axis=0))
        denom = total * jnp.exp2(peak - top) + jnp.sum(
            both[:, 1:2, :] * jnp.exp2(both[:, 0:1, :] - top[None]), axis=0
        )
        lse_ref[:, pl.ds(h * count, count)] = top + jnp.log2(denom)

    start = (jnp.full((1, count), -jnp.inf, jnp.float32), jnp.zeros((1, count), jnp.float32))
    relay_line(0)
    relay_line(1)
    relay_pair(0)
    gathered(0)
    carry0 = stats(0, 0, tiles // 2, start)
    relay_pair(1)
    carry0 = stats(0, tiles // 2, tiles, carry0)
    publish(0, carry0)
    gathered(1)
    carry1 = stats(1, 0, tiles, start)
    publish(1, carry1)
    merge(0, carry0)
    merge(1, carry1)
    others = all_ref.at[pl.ds(0, (n - 1) * rows)]
    pltpu.make_async_copy(others, others, sems.at[0]).wait()
    pltpu.make_async_copy(theirs, theirs, sems.at[1]).wait()


def update_kernel(cen_ref, pts_ref, lse_ref, one_ref, moved_ref, mass_ref):
    tile, width = cen_ref.shape
    cen, pts = cen_ref[...], pts_ref[...]
    logits = lax.dot_general(cen, pts, ROWS_BY_ROWS, preferred_element_type=jnp.float32)
    resp = jnp.exp2(logits * log2_scale(width) - lse_ref[...])
    mass = jnp.sum(resp, axis=1, keepdims=True)
    weighted = jnp.dot(resp.astype(jnp.bfloat16), pts, preferred_element_type=jnp.float32)
    fresh = (weighted + PRIOR_ONE * cen.astype(jnp.float32)) * (1.0 / (mass + PRIOR_ONE))
    one_ref[...] = fresh.astype(jnp.bfloat16)
    moved_ref[...] = (mass * fresh).astype(jnp.bfloat16)
    mass_ref[...] = jnp.broadcast_to(mass, (tile, LANES)).T[0:1, :]


def coarse_kernel(
    n,
    moved_hbm,
    mass_ref,
    assign_ref,
    init_ref,
    two_ref,
    moved,
    sums,
    weights,
    core_out,
    core_in,
    pair_out,
    pair_in,
    line_out,
    line_in,
    held,
    mass_out,
    mass_in,
    moved_sem,
    core_sem,
    pair_sem,
    line_sem,
    mass_sem,
):
    group, me = lax.axis_index("groups"), lax.axis_index("cent")
    own, width = init_ref.shape
    local = moved.shape[0]
    lines = n // 4
    steps = lines.bit_length() - 1
    cuts = 2
    cut = own // cuts
    tile = min(512, local)
    line, pair, core = me // 4, lax.rem(me // 2, 2), lax.rem(me, 2)

    def at(z, y, c):
        return z * 4 + y * 2 + c

    load = pltpu.make_async_copy(moved_hbm, moved, moved_sem)
    load.start()
    barrier = pltpu.get_barrier_semaphore()

    @pl.loop(1, n)
    def _(off):
        peer = lax.rem(me + off, n)
        pl.semaphore_signal(barrier, inc=1, device_id=(group, peer), device_id_type=MESH)

    pl.semaphore_wait(barrier, n - 1)
    load.wait()

    def copy(src, dst, sem, slot, z, y, c):
        return pltpu.make_async_remote_copy(
            src_ref=src,
            dst_ref=dst,
            send_sem=sem.at[(0, *slot)],
            recv_sem=sem.at[(1, *slot)],
            device_id=(group, at(z, y, c)),
            device_id_type=MESH,
        )

    def core_copy(e, q):
        return copy(core_out.at[e, q], core_in.at[e, q], core_sem, (e, q), line, pair, 1 - core)

    def pair_copy(e, h):
        part = pl.ds(h * cut, cut)
        return copy(
            pair_out.at[e, part], pair_in.at[e, part], pair_sem, (e, h), line, 1 - pair, core
        )

    def line_copy(e, h):
        part = pl.ds(h * cut, cut)
        z = flip(line, e & -e, lines)
        return copy(line_out.at[e, part], line_in.at[e, part], line_sem, (e, h), z, pair, core)

    def mass_copy(peer, off):
        return pltpu.make_async_remote_copy(
            src_ref=mass_out.at[peer],
            dst_ref=mass_in.at[off],
            send_sem=mass_sem.at[0],
            recv_sem=mass_sem.at[1],
            device_id=(group, peer),
            device_id_type=MESH,
        )

    row = lax.broadcasted_iota(jnp.int32, (2 * own, 1), 0)

    def partial(e, y):
        z = flip(line, e, lines)
        theirs, ours = at(z, y, 1 - core), at(z, y, core)
        want = jnp.where(row < own, theirs * own + row, ours * own + row - own)
        sums[...] = jnp.zeros_like(sums)
        weights[...] = jnp.zeros_like(weights)

        @pl.loop(0, local // tile)
        def _(t):
            part = pl.ds(pl.multiple_of(t * tile, tile), tile)
            hit = assign_ref[:, part] == want
            value = jnp.where(hit, mass_ref[:, part], 0.0)
            fold = value[:, :LANES]
            for s in range(LANES, tile, LANES):
                fold = fold + value[:, s : s + LANES]
            weights[...] += fold
            onehot = jnp.where(hit, 1.0, 0.0).astype(jnp.bfloat16)
            sums[...] += jnp.dot(onehot, moved[part, :], preferred_element_type=jnp.float32)

        weight = jnp.sum(weights[...], axis=1, keepdims=True)
        flat = jnp.broadcast_to(weight, (2 * own, LANES)).T
        mass_out[theirs] = flat[0:1, :own]
        mass_out[ours] = flat[0:1, own:]

    def first(e):
        partial(e, 1 - pair)
        core_out[e, 0] = sums[:own, :].astype(jnp.bfloat16)
        core_copy(e, 0).start()
        held[e] = sums[own:, :]

    def swap(e):
        core_copy(e, 0).wait_recv()
        for h in range(cuts):
            part = pl.ds(h * cut, cut)
            both = held[e, part, :] + core_in[e, 0, part, :].astype(jnp.float32)
            pair_out[e, part, :] = both.astype(jnp.bfloat16)
            pair_copy(e, h).start()

    def second(e):
        partial(e, pair)
        core_out[e, 1] = sums[:own, :].astype(jnp.bfloat16)
        core_copy(e, 1).start()
        held[e] = sums[own:, :]

    def climb(e):
        core_copy(e, 1).wait_recv()
        for h in range(cuts):
            part = pl.ds(h * cut, cut)
            total = held[e, part, :] + core_in[e, 1, part, :].astype(jnp.float32)
            pair_copy(e, h).wait_recv()
            total = total + pair_in[e, part, :].astype(jnp.float32)
            for i in range(steps):
                if e % (2 << i) == 0:
                    line_copy(e + (1 << i), h).wait_recv()
                    total = total + line_in[e + (1 << i), part, :].astype(jnp.float32)
            if e > 0:
                line_out[e, part, :] = total.astype(jnp.bfloat16)
                line_copy(e, h).start()
            else:
                held[e, part, :] = total

    order = list(range(lines - 1, -1, -1))
    first(order[0])
    for s, e in enumerate(order):
        if s + 1 < lines:
            first(order[s + 1])
        swap(e)
        second(e)
        if s == lines - 1:

            @pl.loop(1, n)
            def _(off):
                mass_copy(lax.rem(me + off, n), off).start()

        if s > 0:
            climb(order[s - 1])
    climb(0)

    rest = mass_in.at[pl.ds(1, n - 1)]
    pltpu.make_async_copy(rest, rest, mass_sem.at[1]).wait()
    mass_in[0] = mass_out[me]
    weight = jnp.sum(mass_in[...], axis=0)
    eye = lax.broadcasted_iota(jnp.int32, (own, own), 0) == lax.broadcasted_iota(
        jnp.int32, (own, own), 1
    )
    weight = jnp.sum(jnp.where(eye, weight, 0.0), axis=1, keepdims=True)
    two_ref[...] = (held[0] + PRIOR_TWO * init_ref[...]) / (weight + PRIOR_TWO)

    for e in range(lines):
        core_copy(e, 0).wait_send()
        core_copy(e, 1).wait_send()
        for h in range(cuts):
            pair_copy(e, h).wait_send()
            if e > 0:
                line_copy(e, h).wait_send()
    pltpu.make_async_copy(rest, rest, mass_sem.at[0]).wait()


def shards(n, points, centroids, coarse_init, assign):
    rows, width = points.shape
    local = centroids.shape[0]
    own = coarse_init.shape[0]
    count = n * rows
    tile = min(512, local)
    lines = n // 4
    vmem = pl.BlockSpec(memory_space=pltpu.VMEM)
    anywhere = pl.BlockSpec(memory_space=pl.ANY)
    everyone, lse = pl.pallas_call(
        functools.partial(stats_kernel, n, tile),
        out_shape=(
            jax.ShapeDtypeStruct((count, width), jnp.bfloat16),
            jax.ShapeDtypeStruct((1, count), jnp.float32),
        ),
        in_specs=[vmem, anywhere],
        out_specs=(vmem, vmem),
        scratch_shapes=[
            pltpu.VMEM((local, width), jnp.bfloat16),
            pltpu.VMEM((2, 2, count // 2), jnp.float32),
            pltpu.VMEM((2, n - 1, 2, count // 2), jnp.float32),
            pltpu.SemaphoreType.DMA((local // tile,)),
            pltpu.SemaphoreType.DMA((2, lines)),
            pltpu.SemaphoreType.DMA((2, lines)),
            pltpu.SemaphoreType.DMA((2,)),
            pltpu.SemaphoreType.DMA((4,)),
        ],
        compiler_params=pltpu.CompilerParams(collective_id=0, has_side_effects=True),
        name="stats",
    )(points, centroids)
    level_one, moved, mass = pl.pallas_call(
        update_kernel,
        grid=(local // tile,),
        out_shape=(
            jax.ShapeDtypeStruct((local, width), jnp.bfloat16),
            jax.ShapeDtypeStruct((local, width), jnp.bfloat16),
            jax.ShapeDtypeStruct((1, local), jnp.float32),
        ),
        in_specs=[
            pl.BlockSpec((tile, width), lambda t: (t, 0)),
            pl.BlockSpec((count, width), lambda t: (0, 0)),
            pl.BlockSpec((1, count), lambda t: (0, 0)),
        ],
        out_specs=(
            pl.BlockSpec((tile, width), lambda t: (t, 0)),
            pl.BlockSpec((tile, width), lambda t: (t, 0)),
            pl.BlockSpec((1, tile), lambda t: (0, t)),
        ),
        name="update",
    )(centroids, everyone, lse)
    level_two = pl.pallas_call(
        functools.partial(coarse_kernel, n),
        out_shape=jax.ShapeDtypeStruct((own, width), jnp.float32),
        in_specs=[anywhere, vmem, vmem, vmem],
        out_specs=vmem,
        scratch_shapes=[
            pltpu.VMEM((local, width), jnp.bfloat16),
            pltpu.VMEM((2 * own, width), jnp.float32),
            pltpu.VMEM((2 * own, LANES), jnp.float32),
            pltpu.VMEM((lines, 2, own, width), jnp.bfloat16),
            pltpu.VMEM((lines, 2, own, width), jnp.bfloat16),
            pltpu.VMEM((lines, own, width), jnp.bfloat16),
            pltpu.VMEM((lines, own, width), jnp.bfloat16),
            pltpu.VMEM((lines, own, width), jnp.bfloat16),
            pltpu.VMEM((lines, own, width), jnp.bfloat16),
            pltpu.VMEM((lines, own, width), jnp.float32),
            pltpu.VMEM((n, 1, own), jnp.float32),
            pltpu.VMEM((n, 1, own), jnp.float32),
            pltpu.SemaphoreType.DMA,
            pltpu.SemaphoreType.DMA((2, lines, 2)),
            pltpu.SemaphoreType.DMA((2, lines, 2)),
            pltpu.SemaphoreType.DMA((2, lines, 2)),
            pltpu.SemaphoreType.DMA((2,)),
        ],
        compiler_params=pltpu.CompilerParams(collective_id=1, has_side_effects=True),
        name="coarse",
    )(moved, mass, assign.reshape(1, local), coarse_init)
    return (level_one, level_two)


def solution(mesh):
    return jax.shard_map(
        functools.partial(shards, mesh.shape["cent"]),
        mesh=mesh,
        in_specs=(
            P(("groups", "cent"), None),
            P(("groups", "cent"), None),
            P(("groups", "cent"), None),
            P(("groups", "cent")),
        ),
        out_specs=(P(("groups", "cent"), None), P(("groups", "cent"), None)),
        check_vma=False,
    )
```

```python
import functools
import math

import jax
import jax.numpy as jnp
from jax import lax
from jax.experimental import pallas as pl
from jax.experimental.pallas import tpu as pltpu
from jax.sharding import PartitionSpec as P

TEMP = 0.05
PRIOR_ONE = 0.02
PRIOR_TWO = 0.25
LANES = 128
VMEM_LIMIT = 24 << 20
MESH = pl.DeviceIdType.MESH
ROWS_BY_ROWS = (((1,), (1,)), ((), ()))


def log2_scale(width):
    return math.log2(math.e) / (TEMP * math.sqrt(width))


def flip(z, e, lines):
    out, bit = 0, 1
    while bit < lines:
        out = out + bit * lax.rem(z // bit + e // bit, 2)
        bit *= 2
    return out


def stats_kernel(
    n,
    tile,
    pts_ref,
    cen,
    all_ref,
    lse_ref,
    logits_ref,
    mine,
    theirs,
    line_sem,
    pair_sem,
    core_sem,
    sems,
):
    group, me = lax.axis_index("groups"), lax.axis_index("cent")
    rows, width = pts_ref.shape
    count = n * rows // 2
    lines = n // 4
    line, pair, core = me // 4, lax.rem(me // 2, 2), lax.rem(me, 2)
    side = line // (lines // 2)
    tiles = cen.shape[0] // tile
    c2 = log2_scale(width)

    barrier = pltpu.get_barrier_semaphore()

    @pl.loop(1, n)
    def _(off):
        peer = lax.rem(me + off, n)
        pl.semaphore_signal(barrier, inc=1, device_id=(group, peer), device_id_type=MESH)

    pl.semaphore_wait(barrier, n - 1)

    def slot(z, y, c):
        return pl.ds(pl.multiple_of((z * 4 + y * 2 + c) * rows, rows), rows)

    def send(src, where, sem, z, y, c):
        return pltpu.make_async_remote_copy(
            src_ref=src,
            dst_ref=all_ref.at[where],
            send_sem=sems.at[0],
            recv_sem=sem,
            device_id=(group, z * 4 + y * 2 + c),
            device_id_type=MESH,
        )

    def along(e, src, where):
        return send(src, where, line_sem.at[e], flip(line, e, lines), pair, core)

    def across(e, src, where):
        return send(src, where, pair_sem.at[e], line, 1 - pair, core)

    def over(e, src, where):
        return send(src, where, core_sem.at[e // (lines // 2)], line, pair, 1 - core)

    def relay_line(e):
        where = slot(flip(line, e, lines), pair, core)
        got = all_ref.at[where]
        along(e, got, where).wait_recv()
        across(e, got, where).start()
        over(e, got, where).start()

    def relay_pair(e):
        where = slot(flip(line, e, lines), 1 - pair, core)
        got = all_ref.at[where]
        across(e, got, where).wait_recv()
        over(e, got, where).start()

    def gathered(h):
        half = all_ref.at[pl.ds(0, count // 2)]
        pltpu.make_async_copy(half, half, core_sem.at[h]).wait()

    where = slot(line, pair, core)
    for e in range(lines - 1, 0, -1):
        along(e, pts_ref, where).start()
    across(0, pts_ref, where).start()
    over(0, pts_ref, where).start()
    all_ref[where, :] = pts_ref[...]

    def at(t, h):
        columns = (side + h - 2 * h * side) * count
        return (
            pl.ds(pl.multiple_of(t * tile, tile), tile),
            pl.ds(pl.multiple_of(columns, count), count),
        )

    def product(t, h, peak):
        rows_of, columns = at(t, h)
        logits = (
            lax.dot_general(
                cen[rows_of, :],
                all_ref[columns, :],
                ROWS_BY_ROWS,
                preferred_element_type=jnp.float32,
            )
            * c2
        )
        logits_ref[rows_of, columns] = logits
        return jnp.maximum(peak, jnp.max(logits.reshape(tile // 8, 8, count), axis=0))

    def exponentials(t, h, peak, total):
        power = jnp.exp2(logits_ref[at(t, h)] - peak)
        return total + jnp.sum(power.reshape(tile // 8, 8, count), axis=0)

    lowest = jnp.full((8, count), -jnp.inf, jnp.float32)
    none = jnp.zeros((8, count), jnp.float32)

    def near(t, peak):
        return product(t, 0, peak)

    def top_of(peak):
        return jnp.max(peak, axis=0, keepdims=True)

    for e in range(1, lines):
        relay_line(e)
    for e in range(lines // 2):
        relay_pair(e)
    gathered(0)
    peak = lowest
    for e in range(lines // 2):
        stop = tiles * (e + 1) // (lines // 2)
        peak = lax.fori_loop(tiles * e // (lines // 2), stop, near, peak)
        relay_pair(lines // 2 + e)
    peak0 = top_of(peak)
    total0 = lax.fori_loop(0, tiles, lambda t, total: exponentials(t, 0, peak0, total), none)
    gathered(1)
    peak1 = top_of(lax.fori_loop(0, tiles, lambda t, peak: product(t, 1, peak), lowest))
    total1 = lax.fori_loop(0, tiles, lambda t, total: exponentials(t, 1, peak1, total), none)
    for h, top, total in ((0, peak0, total0), (1, peak1, total1)):
        columns = at(0, h)[1]
        mine[0:1, columns] = top
        mine[1:2, columns] = jnp.sum(total, axis=0, keepdims=True)

    @pl.loop(1, n)
    def _(off):
        pltpu.make_async_remote_copy(
            src_ref=mine,
            dst_ref=theirs.at[off - 1],
            send_sem=sems.at[1],
            recv_sem=sems.at[2],
            device_id=(group, lax.rem(me + off, n)),
            device_id_type=MESH,
        ).start()

    pltpu.make_async_copy(theirs, theirs, sems.at[2]).wait()
    peak, total = mine[0:1, :], mine[1:2, :]
    both = theirs[...]
    top = jnp.maximum(peak, jnp.max(both[:, 0:1, :], axis=0))
    denom = total * jnp.exp2(peak - top) + jnp.sum(
        both[:, 1:2, :] * jnp.exp2(both[:, 0:1, :] - top[None]), axis=0
    )
    lse_ref[...] = top + jnp.log2(denom)
    others = all_ref.at[pl.ds(0, (n - 1) * rows)]
    pltpu.make_async_copy(others, others, sems.at[0]).wait()
    pltpu.make_async_copy(theirs, theirs, sems.at[1]).wait()


def update_kernel(
    tile, cen_ref, logits_ref, pts_ref, lse_ref, one_hbm, moved_ref, mass_ref, stage, sem
):
    local = cen_ref.shape[0]

    @pl.loop(0, local // tile)
    def _(t):
        rows = pl.ds(pl.multiple_of(t * tile, tile), tile)
        resp = jnp.exp2(logits_ref[rows, :] - lse_ref[...])
        mass = jnp.sum(resp, axis=1, keepdims=True)
        weighted = jnp.dot(
            resp.astype(jnp.bfloat16), pts_ref[...], preferred_element_type=jnp.float32
        )
        fresh = (weighted + PRIOR_ONE * cen_ref[rows, :].astype(jnp.float32)) * (
            1.0 / (mass + PRIOR_ONE)
        )
        stage[rows, :] = fresh.astype(jnp.bfloat16)
        pltpu.make_async_copy(stage.at[rows], one_hbm.at[rows], sem).start()
        moved_ref[rows, :] = (mass * fresh).astype(jnp.bfloat16)
        mass_ref[:, rows] = jnp.broadcast_to(mass, (tile, LANES)).T[0:1, :]

    pltpu.make_async_copy(stage, one_hbm, sem).wait()


def coarse_kernel(
    n,
    moved,
    mass_ref,
    assign_ref,
    init_ref,
    two_ref,
    sums,
    weights,
    core_out,
    core_in,
    pair_out,
    pair_in,
    line_out,
    line_in,
    held,
    mass_out,
    mass_in,
    core_sem,
    pair_sem,
    line_sem,
    mass_sem,
):
    group, me = lax.axis_index("groups"), lax.axis_index("cent")
    own, width = init_ref.shape
    local = moved.shape[0]
    lines = n // 4
    steps = lines.bit_length() - 1
    cuts = 2
    cut = own // cuts
    tile = min(2048, local)
    line, pair, core = me // 4, lax.rem(me // 2, 2), lax.rem(me, 2)

    def at(z, y, c):
        return z * 4 + y * 2 + c

    barrier = pltpu.get_barrier_semaphore()

    @pl.loop(1, n)
    def _(off):
        peer = lax.rem(me + off, n)
        pl.semaphore_signal(barrier, inc=1, device_id=(group, peer), device_id_type=MESH)

    def copy(src, dst, sem, slot, z, y, c):
        return pltpu.make_async_remote_copy(
            src_ref=src,
            dst_ref=dst,
            send_sem=sem.at[(0, *slot)],
            recv_sem=sem.at[(1, *slot)],
            device_id=(group, at(z, y, c)),
            device_id_type=MESH,
        )

    def core_copy(e, q):
        return copy(core_out.at[e, q], core_in.at[e, q], core_sem, (e, q), line, pair, 1 - core)

    def pair_copy(e, h):
        part = pl.ds(h * cut, cut)
        return copy(
            pair_out.at[e, part], pair_in.at[e, part], pair_sem, (e, h), line, 1 - pair, core
        )

    def line_copy(e, h):
        part = pl.ds(h * cut, cut)
        z = flip(line, e & -e, lines)
        return copy(line_out.at[e, part], line_in.at[e, part], line_sem, (e, h), z, pair, core)

    def mass_copy(peer):
        return pltpu.make_async_remote_copy(
            src_ref=mass_out.at[peer],
            dst_ref=mass_in.at[me],
            send_sem=mass_sem.at[0],
            recv_sem=mass_sem.at[1],
            device_id=(group, peer),
            device_id_type=MESH,
        )

    def partial(*owners):
        size = own * len(owners)
        row = lax.broadcasted_iota(jnp.int32, (size, 1), 0)
        want = row + owners[0] * own
        if len(owners) == 2:
            want = jnp.where(row < own, want, row - own + owners[1] * own)
        here = pl.ds(0, size)
        sums[here, :] = jnp.zeros((size, width), jnp.float32)
        weights[here, :] = jnp.zeros((size, LANES), jnp.float32)

        @pl.loop(0, local // tile)
        def _(t):
            part = pl.ds(pl.multiple_of(t * tile, tile), tile)
            hit = assign_ref[:, part] == want
            value = jnp.where(hit, mass_ref[:, part], 0.0)
            fold = value[:, :LANES]
            for s in range(LANES, tile, LANES):
                fold = fold + value[:, s : s + LANES]
            weights[here, :] += fold
            onehot = jnp.where(hit, 1.0, 0.0).astype(jnp.bfloat16)
            sums[here, :] += jnp.dot(onehot, moved[part, :], preferred_element_type=jnp.float32)

        weight = jnp.sum(weights[here, :], axis=1, keepdims=True)
        flat = jnp.broadcast_to(weight, (size, LANES)).T
        for s, owner in enumerate(owners):
            mass_out[owner] = flat[0:1, s * own : (s + 1) * own]

    def both(e, y):
        z = flip(line, e, lines)
        return at(z, y, 1 - core), at(z, y, core)

    def export(e, q):
        core_out[e, q] = sums[:own, :].astype(jnp.bfloat16)
        core_copy(e, q).start()

    def opening(e):
        theirs, ours = both(e, 1 - pair)
        partial(theirs)
        pl.semaphore_wait(barrier, n - 1)
        export(e, 0)
        mass_copy(theirs).start()
        partial(ours)
        mass_copy(ours).start()
        held[e, 0] = sums[:own, :]

    def compute(e, q):
        theirs, ours = both(e, pair if q else 1 - pair)
        partial(theirs, ours)
        export(e, q)
        mass_copy(theirs).start()
        if e > 0 or q == 0:
            mass_copy(ours).start()
        held[e, q] = sums[own:, :]

    def swap(e):
        core_copy(e, 0).wait_recv()
        for h in range(cuts):
            part = pl.ds(h * cut, cut)
            total = held[e, 0, part, :] + core_in[e, 0, part, :].astype(jnp.float32)
            pair_out[e, part, :] = total.astype(jnp.bfloat16)
            pair_copy(e, h).start()

    def climb(e, h):
        if h == 0:
            core_copy(e, 1).wait_recv()
        part = pl.ds(h * cut, cut)
        total = held[e, 1, part, :] + core_in[e, 1, part, :].astype(jnp.float32)
        pair_copy(e, h).wait_recv()
        total = total + pair_in[e, part, :].astype(jnp.float32)
        for i in range(steps):
            if e % (2 << i) == 0:
                line_copy(e + (1 << i), h).wait_recv()
                total = total + line_in[e + (1 << i), part, :].astype(jnp.float32)
        if e > 0:
            line_out[e, part, :] = total.astype(jnp.bfloat16)
            line_copy(e, h).start()
        else:
            held[e, 1, part, :] = total

    order = list(range(lines - 1, -1, -1))
    opening(order[0])
    swap(order[0])
    for s, e in enumerate(order):
        if s + 1 < lines:
            compute(order[s + 1], 0)
        if s > 0:
            climb(order[s - 1], 1)
        compute(e, 1)
        if s + 1 < lines:
            swap(order[s + 1])
        climb(e, 0)
    climb(0, 1)

    rest = mass_in.at[pl.ds(1, n - 1)]
    pltpu.make_async_copy(rest, rest, mass_sem.at[1]).wait()
    mass_in[me] = mass_out[me]
    weight = jnp.sum(mass_in[...], axis=0)
    eye = lax.broadcasted_iota(jnp.int32, (own, own), 0) == lax.broadcasted_iota(
        jnp.int32, (own, own), 1
    )
    weight = jnp.sum(jnp.where(eye, weight, 0.0), axis=1, keepdims=True)
    two_ref[...] = (held[0, 1] + PRIOR_TWO * init_ref[...]) / (weight + PRIOR_TWO)

    for e in range(lines):
        core_copy(e, 0).wait_send()
        core_copy(e, 1).wait_send()
        for h in range(cuts):
            pair_copy(e, h).wait_send()
            if e > 0:
                line_copy(e, h).wait_send()
    pltpu.make_async_copy(rest, rest, mass_sem.at[0]).wait()


def shards(n, points, centroids, coarse_init, assign):
    rows, width = points.shape
    local = centroids.shape[0]
    own = coarse_init.shape[0]
    count = n * rows
    tile = min(1024, local)
    lines = n // 4
    vmem = pl.BlockSpec(memory_space=pltpu.VMEM)
    anywhere = pl.BlockSpec(memory_space=pl.ANY)
    everyone, lse, logits = pl.pallas_call(
        functools.partial(stats_kernel, n, tile),
        out_shape=(
            jax.ShapeDtypeStruct((count, width), jnp.bfloat16),
            jax.ShapeDtypeStruct((1, count), jnp.float32),
            jax.ShapeDtypeStruct((local, count), jnp.float32),
        ),
        in_specs=[vmem, vmem],
        out_specs=(vmem, vmem, vmem),
        scratch_shapes=[
            pltpu.VMEM((2, count), jnp.float32),
            pltpu.VMEM((n - 1, 2, count), jnp.float32),
            pltpu.SemaphoreType.DMA((lines,)),
            pltpu.SemaphoreType.DMA((lines,)),
            pltpu.SemaphoreType.DMA((2,)),
            pltpu.SemaphoreType.DMA((3,)),
        ],
        compiler_params=pltpu.CompilerParams(
            collective_id=0, has_side_effects=True, vmem_limit_bytes=VMEM_LIMIT
        ),
        name="stats",
    )(points, centroids)
    chunk = min(local, max(64, tile * 256 // count))
    level_one, moved, mass = pl.pallas_call(
        functools.partial(update_kernel, chunk),
        out_shape=(
            jax.ShapeDtypeStruct((local, width), jnp.bfloat16),
            jax.ShapeDtypeStruct((local, width), jnp.bfloat16),
            jax.ShapeDtypeStruct((1, local), jnp.float32),
        ),
        in_specs=[vmem, vmem, vmem, vmem],
        out_specs=(anywhere, vmem, vmem),
        scratch_shapes=[
            pltpu.VMEM((local, width), jnp.bfloat16),
            pltpu.SemaphoreType.DMA,
        ],
        compiler_params=pltpu.CompilerParams(vmem_limit_bytes=VMEM_LIMIT),
        name="update",
    )(centroids, logits, everyone, lse)
    level_two = pl.pallas_call(
        functools.partial(coarse_kernel, n),
        out_shape=jax.ShapeDtypeStruct((own, width), jnp.float32),
        in_specs=[vmem, vmem, vmem, vmem],
        out_specs=vmem,
        scratch_shapes=[
            pltpu.VMEM((2 * own, width), jnp.float32),
            pltpu.VMEM((2 * own, LANES), jnp.float32),
            pltpu.VMEM((lines, 2, own, width), jnp.bfloat16),
            pltpu.VMEM((lines, 2, own, width), jnp.bfloat16),
            pltpu.VMEM((lines, own, width), jnp.bfloat16),
            pltpu.VMEM((lines, own, width), jnp.bfloat16),
            pltpu.VMEM((lines, own, width), jnp.bfloat16),
            pltpu.VMEM((lines, own, width), jnp.bfloat16),
            pltpu.VMEM((lines, 2, own, width), jnp.float32),
            pltpu.VMEM((n, 1, own), jnp.float32),
            pltpu.VMEM((n, 1, own), jnp.float32),
            pltpu.SemaphoreType.DMA((2, lines, 2)),
            pltpu.SemaphoreType.DMA((2, lines, 2)),
            pltpu.SemaphoreType.DMA((2, lines, 2)),
            pltpu.SemaphoreType.DMA((2,)),
        ],
        compiler_params=pltpu.CompilerParams(
            collective_id=1, has_side_effects=True, vmem_limit_bytes=VMEM_LIMIT
        ),
        name="coarse",
    )(moved, mass, assign.reshape(1, local), coarse_init)
    return (level_one, level_two)


def solution(mesh):
    return jax.shard_map(
        functools.partial(shards, mesh.shape["cent"]),
        mesh=mesh,
        in_specs=(
            P(("groups", "cent"), None),
            P(("groups", "cent"), None),
            P(("groups", "cent"), None),
            P(("groups", "cent")),
        ),
        out_specs=(P(("groups", "cent"), None), P(("groups", "cent"), None)),
        check_vma=False,
    )
```

```python
import functools
import math

import jax
import jax.numpy as jnp
from jax import lax
from jax.experimental import pallas as pl
from jax.experimental.pallas import tpu as pltpu
from jax.sharding import PartitionSpec as P

TEMP = 0.05
PRIOR_ONE = 0.02
PRIOR_TWO = 0.25
LANES = 128
VMEM_LIMIT = 24 << 20
MESH = pl.DeviceIdType.MESH
ROWS_BY_ROWS = (((1,), (1,)), ((), ()))


def log2_scale(width):
    return math.log2(math.e) / (TEMP * math.sqrt(width))


def flip(z, e, lines):
    out, bit = 0, 1
    while bit < lines:
        out = out + bit * lax.rem(z // bit + e // bit, 2)
        bit *= 2
    return out


def stats_kernel(
    n,
    tile,
    pts_ref,
    cen,
    all_ref,
    lse_ref,
    logits_ref,
    mine,
    theirs,
    line_sem,
    pair_sem,
    core_sem,
    sems,
):
    group, me = lax.axis_index("groups"), lax.axis_index("cent")
    rows, width = pts_ref.shape
    count = n * rows // 2
    lines = n // 4
    line, pair, core = me // 4, lax.rem(me // 2, 2), lax.rem(me, 2)
    side = line // (lines // 2)
    tiles = cen.shape[0] // tile
    c2 = log2_scale(width)

    barrier = pltpu.get_barrier_semaphore()

    @pl.loop(1, n)
    def _(off):
        peer = lax.rem(me + off, n)
        pl.semaphore_signal(barrier, inc=1, device_id=(group, peer), device_id_type=MESH)

    pl.semaphore_wait(barrier, n - 1)

    def slot(z, y, c):
        return pl.ds(pl.multiple_of((z * 4 + y * 2 + c) * rows, rows), rows)

    def send(src, where, sem, z, y, c):
        return pltpu.make_async_remote_copy(
            src_ref=src,
            dst_ref=all_ref.at[where],
            send_sem=sems.at[0],
            recv_sem=sem,
            device_id=(group, z * 4 + y * 2 + c),
            device_id_type=MESH,
        )

    def along(e, src, where):
        return send(src, where, line_sem.at[e], flip(line, e, lines), pair, core)

    def across(e, src, where):
        return send(src, where, pair_sem.at[e], line, 1 - pair, core)

    def over(e, src, where):
        return send(src, where, core_sem.at[e // (lines // 2)], line, pair, 1 - core)

    def relay_line(e):
        where = slot(flip(line, e, lines), pair, core)
        got = all_ref.at[where]
        along(e, got, where).wait_recv()
        across(e, got, where).start()
        over(e, got, where).start()

    def relay_pair(e):
        where = slot(flip(line, e, lines), 1 - pair, core)
        got = all_ref.at[where]
        across(e, got, where).wait_recv()
        over(e, got, where).start()

    def gathered(h):
        half = all_ref.at[pl.ds(0, count // 2)]
        pltpu.make_async_copy(half, half, core_sem.at[h]).wait()

    where = slot(line, pair, core)
    for e in range(lines - 1, 0, -1):
        along(e, pts_ref, where).start()
    across(0, pts_ref, where).start()
    over(0, pts_ref, where).start()
    all_ref[where, :] = pts_ref[...]

    def at(t, h):
        columns = (side + h - 2 * h * side) * count
        return (
            pl.ds(pl.multiple_of(t * tile, tile), tile),
            pl.ds(pl.multiple_of(columns, count), count),
        )

    def product(t, h, peak):
        rows_of, columns = at(t, h)
        logits = (
            lax.dot_general(
                cen[rows_of, :],
                all_ref[columns, :],
                ROWS_BY_ROWS,
                preferred_element_type=jnp.float32,
            )
            * c2
        )
        logits_ref[rows_of, columns] = logits
        return jnp.maximum(peak, jnp.max(logits.reshape(tile // 8, 8, count), axis=0))

    def exponentials(t, h, peak, total):
        power = jnp.exp2(logits_ref[at(t, h)] - peak)
        return total + jnp.sum(power.reshape(tile // 8, 8, count), axis=0)

    lowest = jnp.full((8, count), -jnp.inf, jnp.float32)
    none = jnp.zeros((8, count), jnp.float32)

    def near(t, peak):
        return product(t, 0, peak)

    def top_of(peak):
        return jnp.max(peak, axis=0, keepdims=True)

    for e in range(1, lines):
        relay_line(e)
    for e in range(lines // 2):
        relay_pair(e)
    gathered(0)
    peak = lowest
    for e in range(lines // 2):
        stop = tiles * (e + 1) // (lines // 2)
        peak = lax.fori_loop(tiles * e // (lines // 2), stop, near, peak)
        relay_pair(lines // 2 + e)
    peak0 = top_of(peak)
    total0 = lax.fori_loop(0, tiles, lambda t, total: exponentials(t, 0, peak0, total), none)
    gathered(1)
    peak1 = top_of(lax.fori_loop(0, tiles, lambda t, peak: product(t, 1, peak), lowest))
    total1 = lax.fori_loop(0, tiles, lambda t, total: exponentials(t, 1, peak1, total), none)
    for h, top, total in ((0, peak0, total0), (1, peak1, total1)):
        columns = at(0, h)[1]
        mine[0:1, columns] = top
        mine[1:2, columns] = jnp.sum(total, axis=0, keepdims=True)

    @pl.loop(1, n)
    def _(off):
        pltpu.make_async_remote_copy(
            src_ref=mine,
            dst_ref=theirs.at[off - 1],
            send_sem=sems.at[1],
            recv_sem=sems.at[2],
            device_id=(group, lax.rem(me + off, n)),
            device_id_type=MESH,
        ).start()

    pltpu.make_async_copy(theirs, theirs, sems.at[2]).wait()
    peak, total = mine[0:1, :], mine[1:2, :]
    both = theirs[...]
    top = jnp.maximum(peak, jnp.max(both[:, 0:1, :], axis=0))
    denom = total * jnp.exp2(peak - top) + jnp.sum(
        both[:, 1:2, :] * jnp.exp2(both[:, 0:1, :] - top[None]), axis=0
    )
    lse_ref[...] = top + jnp.log2(denom)
    others = all_ref.at[pl.ds(0, (n - 1) * rows)]
    pltpu.make_async_copy(others, others, sems.at[0]).wait()
    pltpu.make_async_copy(theirs, theirs, sems.at[1]).wait()


def update_kernel(
    tile, cen_ref, logits_ref, pts_ref, lse_ref, one_hbm, moved_ref, mass_ref, stage, sem
):
    local = cen_ref.shape[0]

    @pl.loop(0, local // tile)
    def _(t):
        rows = pl.ds(pl.multiple_of(t * tile, tile), tile)
        resp = jnp.exp2(logits_ref[rows, :] - lse_ref[...])
        mass = jnp.sum(resp, axis=1, keepdims=True)
        weighted = jnp.dot(
            resp.astype(jnp.bfloat16), pts_ref[...], preferred_element_type=jnp.float32
        )
        fresh = (weighted + PRIOR_ONE * cen_ref[rows, :].astype(jnp.float32)) * (
            1.0 / (mass + PRIOR_ONE)
        )
        stage[rows, :] = fresh.astype(jnp.bfloat16)
        pltpu.make_async_copy(stage.at[rows], one_hbm.at[rows], sem).start()
        moved_ref[rows, :] = (mass * fresh).astype(jnp.bfloat16)
        mass_ref[:, rows] = jnp.broadcast_to(mass, (tile, LANES)).T[0:1, :]

    pltpu.make_async_copy(stage, one_hbm, sem).wait()


def coarse_kernel(
    n,
    moved,
    mass_ref,
    assign_ref,
    init_ref,
    two_ref,
    sums,
    weights,
    core_out,
    core_in,
    pair_out,
    pair_in,
    line_out,
    line_in,
    held,
    mass_out,
    mass_in,
    core_sem,
    pair_sem,
    line_sem,
    mass_sem,
):
    group, me = lax.axis_index("groups"), lax.axis_index("cent")
    own, width = init_ref.shape
    local = moved.shape[0]
    lines = n // 4
    steps = lines.bit_length() - 1
    cuts = 2
    cut = own // cuts
    tile = min(2048, local)
    line, pair, core = me // 4, lax.rem(me // 2, 2), lax.rem(me, 2)

    def at(z, y, c):
        return z * 4 + y * 2 + c

    barrier = pltpu.get_barrier_semaphore()

    @pl.loop(1, n)
    def _(off):
        peer = lax.rem(me + off, n)
        pl.semaphore_signal(barrier, inc=1, device_id=(group, peer), device_id_type=MESH)

    def copy(src, dst, sem, slot, z, y, c):
        return pltpu.make_async_remote_copy(
            src_ref=src,
            dst_ref=dst,
            send_sem=sem.at[(0, *slot)],
            recv_sem=sem.at[(1, *slot)],
            device_id=(group, at(z, y, c)),
            device_id_type=MESH,
        )

    def core_copy(e, q):
        return copy(core_out.at[e, q], core_in.at[e, q], core_sem, (e, q), line, pair, 1 - core)

    def pair_copy(e, h):
        part = pl.ds(h * cut, cut)
        return copy(
            pair_out.at[e, part], pair_in.at[e, part], pair_sem, (e, h), line, 1 - pair, core
        )

    forward = lines == 4
    inner = lax.rem(line // 2 + line, 2) == 1

    def line_copy(e, h, away=None):
        part = pl.ds(h * cut, cut)
        z = flip(line, e & -e if away is None else away, lines)
        return copy(line_out.at[e, part], line_in.at[e, part], line_sem, (e, h), z, pair, core)

    def mass_copy(peer):
        return pltpu.make_async_remote_copy(
            src_ref=mass_out.at[peer],
            dst_ref=mass_in.at[me],
            send_sem=mass_sem.at[0],
            recv_sem=mass_sem.at[1],
            device_id=(group, peer),
            device_id_type=MESH,
        )

    def partial(*owners):
        size = own * len(owners)
        row = lax.broadcasted_iota(jnp.int32, (size, 1), 0)
        want = row + owners[0] * own
        if len(owners) == 2:
            want = jnp.where(row < own, want, row - own + owners[1] * own)
        here = pl.ds(0, size)
        sums[here, :] = jnp.zeros((size, width), jnp.float32)
        weights[here, :] = jnp.zeros((size, LANES), jnp.float32)

        @pl.loop(0, local // tile)
        def _(t):
            part = pl.ds(pl.multiple_of(t * tile, tile), tile)
            hit = assign_ref[:, part] == want
            value = jnp.where(hit, mass_ref[:, part], 0.0)
            fold = value[:, :LANES]
            for s in range(LANES, tile, LANES):
                fold = fold + value[:, s : s + LANES]
            weights[here, :] += fold
            onehot = jnp.where(hit, 1.0, 0.0).astype(jnp.bfloat16)
            sums[here, :] += jnp.dot(onehot, moved[part, :], preferred_element_type=jnp.float32)

        weight = jnp.sum(weights[here, :], axis=1, keepdims=True)
        flat = jnp.broadcast_to(weight, (size, LANES)).T
        for s, owner in enumerate(owners):
            mass_out[owner] = flat[0:1, s * own : (s + 1) * own]

    def both(e, y):
        z = flip(line, e, lines)
        return at(z, y, 1 - core), at(z, y, core)

    def export(e, q):
        core_out[e, q] = sums[:own, :].astype(jnp.bfloat16)
        core_copy(e, q).start()

    def opening(e):
        theirs, ours = both(e, 1 - pair)
        partial(theirs)
        pl.semaphore_wait(barrier, n - 1)
        export(e, 0)
        mass_copy(theirs).start()
        partial(ours)
        mass_copy(ours).start()
        held[e, 0] = sums[:own, :]

    def compute(e, q):
        theirs, ours = both(e, pair if q else 1 - pair)
        partial(theirs, ours)
        export(e, q)
        mass_copy(theirs).start()
        if e > 0 or q == 0:
            mass_copy(ours).start()
        held[e, q] = sums[own:, :]

    def swap(e):
        core_copy(e, 0).wait_recv()
        for h in range(cuts):
            part = pl.ds(h * cut, cut)
            total = held[e, 0, part, :] + core_in[e, 0, part, :].astype(jnp.float32)
            pair_out[e, part, :] = total.astype(jnp.bfloat16)
            pair_copy(e, h).start()

    def base(e, h):
        if h == 0:
            core_copy(e, 1).wait_recv()
        part = pl.ds(h * cut, cut)
        total = held[e, 1, part, :] + core_in[e, 1, part, :].astype(jnp.float32)
        pair_copy(e, h).wait_recv()
        return total + pair_in[e, part, :].astype(jnp.float32)

    def pass_on(slot, h, away, total):
        line_out[slot, pl.ds(h * cut, cut), :] = total.astype(jnp.bfloat16)
        line_copy(slot, h, away).start()

    def arrived(slot, h):
        line_copy(slot, h, 1).wait_recv()
        return line_in[slot, pl.ds(h * cut, cut), :].astype(jnp.float32)

    def climb_four(e, h):
        part = pl.ds(h * cut, cut)
        if e == 1:

            @pl.when(inner)
            def _():
                pass_on(0, h, 3, held[3, 1, part, :] + arrived(2, h))

        held[e, 1, part, :] = base(e, h)
        if e == 0:
            held[e, 1, part, :] += arrived(1, h)

        @pl.when(inner)
        def _():
            if e == 2:
                pass_on(2, h, 2, held[e, 1, part, :] + arrived(3, h))
            elif e == 1:
                pass_on(1, h, 1, held[e, 1, part, :])
            elif e == 0:
                held[e, 1, part, :] += arrived(0, h)

        @pl.when(jnp.logical_not(inner))
        def _():
            if e > 0:
                pass_on(e, h, 1, held[e, 1, part, :])
            else:
                held[e, 1, part, :] += arrived(2, h)

    def climb(e, h):
        if forward:
            climb_four(e, h)
            return
        part = pl.ds(h * cut, cut)
        total = base(e, h)
        for i in range(steps):
            if e % (2 << i) == 0:
                line_copy(e + (1 << i), h).wait_recv()
                total = total + line_in[e + (1 << i), part, :].astype(jnp.float32)
        if e > 0:
            line_out[e, part, :] = total.astype(jnp.bfloat16)
            line_copy(e, h).start()
        else:
            held[e, 1, part, :] = total

    order = list(range(lines - 1, -1, -1))
    opening(order[0])
    swap(order[0])
    for s, e in enumerate(order):
        if s + 1 < lines:
            compute(order[s + 1], 0)
        if s > 0:
            climb(order[s - 1], 1)
        compute(e, 1)
        if s + 1 < lines:
            swap(order[s + 1])
        climb(e, 0)
    climb(0, 1)

    rest = mass_in.at[pl.ds(1, n - 1)]
    pltpu.make_async_copy(rest, rest, mass_sem.at[1]).wait()
    mass_in[me] = mass_out[me]
    weight = jnp.sum(mass_in[...], axis=0)
    eye = lax.broadcasted_iota(jnp.int32, (own, own), 0) == lax.broadcasted_iota(
        jnp.int32, (own, own), 1
    )
    weight = jnp.sum(jnp.where(eye, weight, 0.0), axis=1, keepdims=True)
    two_ref[...] = (held[0, 1] + PRIOR_TWO * init_ref[...]) / (weight + PRIOR_TWO)

    for e in range(lines):
        core_copy(e, 0).wait_send()
        core_copy(e, 1).wait_send()
        for h in range(cuts):
            pair_copy(e, h).wait_send()
            if forward and e in (0, 3):

                @pl.when(inner if e == 0 else jnp.logical_not(inner))
                def _(e=e, h=h):
                    line_copy(e, h, 1).wait_send()

            elif e > 0:
                line_copy(e, h).wait_send()
    pltpu.make_async_copy(rest, rest, mass_sem.at[0]).wait()


def shards(n, points, centroids, coarse_init, assign):
    rows, width = points.shape
    local = centroids.shape[0]
    own = coarse_init.shape[0]
    count = n * rows
    tile = min(1024, local)
    lines = n // 4
    vmem = pl.BlockSpec(memory_space=pltpu.VMEM)
    anywhere = pl.BlockSpec(memory_space=pl.ANY)
    everyone, lse, logits = pl.pallas_call(
        functools.partial(stats_kernel, n, tile),
        out_shape=(
            jax.ShapeDtypeStruct((count, width), jnp.bfloat16),
            jax.ShapeDtypeStruct((1, count), jnp.float32),
            jax.ShapeDtypeStruct((local, count), jnp.float32),
        ),
        in_specs=[vmem, vmem],
        out_specs=(vmem, vmem, vmem),
        scratch_shapes=[
            pltpu.VMEM((2, count), jnp.float32),
            pltpu.VMEM((n - 1, 2, count), jnp.float32),
            pltpu.SemaphoreType.DMA((lines,)),
            pltpu.SemaphoreType.DMA((lines,)),
            pltpu.SemaphoreType.DMA((2,)),
            pltpu.SemaphoreType.DMA((3,)),
        ],
        compiler_params=pltpu.CompilerParams(
            collective_id=0, has_side_effects=True, vmem_limit_bytes=VMEM_LIMIT
        ),
        name="stats",
    )(points, centroids)
    chunk = min(local, max(64, tile * 256 // count))
    level_one, moved, mass = pl.pallas_call(
        functools.partial(update_kernel, chunk),
        out_shape=(
            jax.ShapeDtypeStruct((local, width), jnp.bfloat16),
            jax.ShapeDtypeStruct((local, width), jnp.bfloat16),
            jax.ShapeDtypeStruct((1, local), jnp.float32),
        ),
        in_specs=[vmem, vmem, vmem, vmem],
        out_specs=(anywhere, vmem, vmem),
        scratch_shapes=[
            pltpu.VMEM((local, width), jnp.bfloat16),
            pltpu.SemaphoreType.DMA,
        ],
        compiler_params=pltpu.CompilerParams(vmem_limit_bytes=VMEM_LIMIT),
        name="update",
    )(centroids, logits, everyone, lse)
    level_two = pl.pallas_call(
        functools.partial(coarse_kernel, n),
        out_shape=jax.ShapeDtypeStruct((own, width), jnp.float32),
        in_specs=[vmem, vmem, vmem, vmem],
        out_specs=vmem,
        scratch_shapes=[
            pltpu.VMEM((2 * own, width), jnp.float32),
            pltpu.VMEM((2 * own, LANES), jnp.float32),
            pltpu.VMEM((lines, 2, own, width), jnp.bfloat16),
            pltpu.VMEM((lines, 2, own, width), jnp.bfloat16),
            pltpu.VMEM((lines, own, width), jnp.bfloat16),
            pltpu.VMEM((lines, own, width), jnp.bfloat16),
            pltpu.VMEM((lines, own, width), jnp.bfloat16),
            pltpu.VMEM((lines, own, width), jnp.bfloat16),
            pltpu.VMEM((lines, 2, own, width), jnp.float32),
            pltpu.VMEM((n, 1, own), jnp.float32),
            pltpu.VMEM((n, 1, own), jnp.float32),
            pltpu.SemaphoreType.DMA((2, lines, 2)),
            pltpu.SemaphoreType.DMA((2, lines, 2)),
            pltpu.SemaphoreType.DMA((2, lines, 2)),
            pltpu.SemaphoreType.DMA((2,)),
        ],
        compiler_params=pltpu.CompilerParams(
            collective_id=1, has_side_effects=True, vmem_limit_bytes=VMEM_LIMIT
        ),
        name="coarse",
    )(moved, mass, assign.reshape(1, local), coarse_init)
    return (level_one, level_two)


def solution(mesh):
    return jax.shard_map(
        functools.partial(shards, mesh.shape["cent"]),
        mesh=mesh,
        in_specs=(
            P(("groups", "cent"), None),
            P(("groups", "cent"), None),
            P(("groups", "cent"), None),
            P(("groups", "cent")),
        ),
        out_specs=(P(("groups", "cent"), None), P(("groups", "cent"), None)),
        check_vma=False,
    )
```

```python
import functools
import math

import jax
import jax.numpy as jnp
from jax import lax
from jax.experimental import pallas as pl
from jax.experimental.pallas import tpu as pltpu
from jax.sharding import PartitionSpec as P

TEMP = 0.05
PRIOR_ONE = 0.02
PRIOR_TWO = 0.25
LANES = 128
VMEM_LIMIT = 24 << 20
MESH = pl.DeviceIdType.MESH
ROWS_BY_ROWS = (((1,), (1,)), ((), ()))


def log2_scale(width):
    return math.log2(math.e) / (TEMP * math.sqrt(width))


def flip(z, e, lines):
    out, bit = 0, 1
    while bit < lines:
        out = out + bit * lax.rem(z // bit + e // bit, 2)
        bit *= 2
    return out


def stats_kernel(
    n,
    tile,
    pts_ref,
    cen,
    all_ref,
    lse_ref,
    logits_ref,
    mine,
    theirs,
    line_sem,
    pair_sem,
    core_sem,
    sems,
):
    group, me = lax.axis_index("groups"), lax.axis_index("cent")
    rows, width = pts_ref.shape
    count = n * rows // 2
    lines = n // 4
    line, pair, core = me // 4, lax.rem(me // 2, 2), lax.rem(me, 2)
    side = line // (lines // 2)
    tiles = cen.shape[0] // tile
    c2 = log2_scale(width)

    barrier = pltpu.get_barrier_semaphore()

    @pl.loop(1, n)
    def _(off):
        peer = lax.rem(me + off, n)
        pl.semaphore_signal(barrier, inc=1, device_id=(group, peer), device_id_type=MESH)

    pl.semaphore_wait(barrier, n - 1)

    def slot(z, y, c):
        return pl.ds(pl.multiple_of((z * 4 + y * 2 + c) * rows, rows), rows)

    def send(src, where, sem, z, y, c):
        return pltpu.make_async_remote_copy(
            src_ref=src,
            dst_ref=all_ref.at[where],
            send_sem=sems.at[0],
            recv_sem=sem,
            device_id=(group, z * 4 + y * 2 + c),
            device_id_type=MESH,
        )

    def along(e, src, where):
        return send(src, where, line_sem.at[e], flip(line, e, lines), pair, core)

    def across(e, src, where):
        return send(src, where, pair_sem.at[e], line, 1 - pair, core)

    def over(e, src, where):
        return send(src, where, core_sem.at[e // (lines // 2)], line, pair, 1 - core)

    def relay_line(e):
        where = slot(flip(line, e, lines), pair, core)
        got = all_ref.at[where]
        along(e, got, where).wait_recv()
        across(e, got, where).start()
        over(e, got, where).start()

    def relay_pair(e):
        where = slot(flip(line, e, lines), 1 - pair, core)
        got = all_ref.at[where]
        across(e, got, where).wait_recv()
        over(e, got, where).start()

    def gathered(h):
        half = all_ref.at[pl.ds(0, count // 2)]
        pltpu.make_async_copy(half, half, core_sem.at[h]).wait()

    where = slot(line, pair, core)
    for e in range(lines - 1, 0, -1):
        along(e, pts_ref, where).start()
    across(0, pts_ref, where).start()
    over(0, pts_ref, where).start()
    all_ref[where, :] = pts_ref[...]

    def at(t, h):
        columns = (side + h - 2 * h * side) * count
        return (
            pl.ds(pl.multiple_of(t * tile, tile), tile),
            pl.ds(pl.multiple_of(columns, count), count),
        )

    def product(t, h, peak):
        rows_of, columns = at(t, h)
        logits = (
            lax.dot_general(
                cen[rows_of, :],
                all_ref[columns, :],
                ROWS_BY_ROWS,
                preferred_element_type=jnp.float32,
            )
            * c2
        )
        logits_ref[rows_of, columns] = logits
        return jnp.maximum(peak, jnp.max(logits.reshape(tile // 8, 8, count), axis=0))

    def exponentials(t, h, peak, total):
        power = jnp.exp2(logits_ref[at(t, h)] - peak)
        return total + jnp.sum(power.reshape(tile // 8, 8, count), axis=0)

    lowest = jnp.full((8, count), -jnp.inf, jnp.float32)
    none = jnp.zeros((8, count), jnp.float32)

    def near(t, peak):
        return product(t, 0, peak)

    def top_of(peak):
        return jnp.max(peak, axis=0, keepdims=True)

    for e in range(1, lines):
        relay_line(e)
    for e in range(lines // 2):
        relay_pair(e)
    gathered(0)
    peak = lowest
    for e in range(lines // 2):
        stop = tiles * (e + 1) // (lines // 2)
        peak = lax.fori_loop(tiles * e // (lines // 2), stop, near, peak)
        relay_pair(lines // 2 + e)
    peak0 = top_of(peak)
    total0 = lax.fori_loop(0, tiles, lambda t, total: exponentials(t, 0, peak0, total), none)
    gathered(1)
    peak1 = top_of(lax.fori_loop(0, tiles, lambda t, peak: product(t, 1, peak), lowest))
    total1 = lax.fori_loop(0, tiles, lambda t, total: exponentials(t, 1, peak1, total), none)
    for h, top, total in ((0, peak0, total0), (1, peak1, total1)):
        columns = at(0, h)[1]
        mine[0:1, columns] = top
        mine[1:2, columns] = jnp.sum(total, axis=0, keepdims=True)

    @pl.loop(1, n)
    def _(off):
        pltpu.make_async_remote_copy(
            src_ref=mine,
            dst_ref=theirs.at[off - 1],
            send_sem=sems.at[1],
            recv_sem=sems.at[2],
            device_id=(group, lax.rem(me + off, n)),
            device_id_type=MESH,
        ).start()

    pltpu.make_async_copy(theirs, theirs, sems.at[2]).wait()
    peak, total = mine[0:1, :], mine[1:2, :]
    both = theirs[...]
    top = jnp.maximum(peak, jnp.max(both[:, 0:1, :], axis=0))
    denom = total * jnp.exp2(peak - top) + jnp.sum(
        both[:, 1:2, :] * jnp.exp2(both[:, 0:1, :] - top[None]), axis=0
    )
    lse_ref[...] = top + jnp.log2(denom)
    others = all_ref.at[pl.ds(0, (n - 1) * rows)]
    pltpu.make_async_copy(others, others, sems.at[0]).wait()
    pltpu.make_async_copy(theirs, theirs, sems.at[1]).wait()


def update_kernel(
    tile, cen_ref, logits_ref, pts_ref, lse_ref, one_hbm, moved_ref, mass_ref, stage, sem
):
    local = cen_ref.shape[0]

    @pl.loop(0, local // tile)
    def _(t):
        rows = pl.ds(pl.multiple_of(t * tile, tile), tile)
        resp = jnp.exp2(logits_ref[rows, :] - lse_ref[...])
        mass = jnp.sum(resp, axis=1, keepdims=True)
        weighted = jnp.dot(
            resp.astype(jnp.bfloat16), pts_ref[...], preferred_element_type=jnp.float32
        )
        fresh = (weighted + PRIOR_ONE * cen_ref[rows, :].astype(jnp.float32)) * (
            1.0 / (mass + PRIOR_ONE)
        )
        stage[rows, :] = fresh.astype(jnp.bfloat16)
        pltpu.make_async_copy(stage.at[rows], one_hbm.at[rows], sem).start()
        moved_ref[rows, :] = (mass * fresh).astype(jnp.bfloat16)
        mass_ref[:, rows] = jnp.broadcast_to(mass, (tile, LANES)).T[0:1, :]

    pltpu.make_async_copy(stage, one_hbm, sem).wait()


def coarse_kernel(
    n,
    moved,
    mass_ref,
    assign_ref,
    init_ref,
    two_ref,
    sums,
    weights,
    core_out,
    core_in,
    pair_out,
    pair_in,
    line_out,
    line_in,
    held,
    mass_out,
    mass_in,
    core_sem,
    pair_sem,
    line_sem,
    mass_sem,
):
    group, me = lax.axis_index("groups"), lax.axis_index("cent")
    own, width = init_ref.shape
    local = moved.shape[0]
    lines = n // 4
    steps = lines.bit_length() - 1
    cuts = 2
    cut = own // cuts
    tile = min(2048, local)
    line, pair, core = me // 4, lax.rem(me // 2, 2), lax.rem(me, 2)

    def at(z, y, c):
        return z * 4 + y * 2 + c

    barrier = pltpu.get_barrier_semaphore()

    @pl.loop(1, n)
    def _(off):
        peer = lax.rem(me + off, n)
        pl.semaphore_signal(barrier, inc=1, device_id=(group, peer), device_id_type=MESH)

    def copy(src, dst, sem, slot, z, y, c):
        return pltpu.make_async_remote_copy(
            src_ref=src,
            dst_ref=dst,
            send_sem=sem.at[(0, *slot)],
            recv_sem=sem.at[(1, *slot)],
            device_id=(group, at(z, y, c)),
            device_id_type=MESH,
        )

    def core_copy(e, q):
        return copy(core_out.at[e, q], core_in.at[e, q], core_sem, (e, q), line, pair, 1 - core)

    def pair_copy(e, h):
        part = pl.ds(h * cut, cut)
        return copy(
            pair_out.at[e, part], pair_in.at[e, part], pair_sem, (e, h), line, 1 - pair, core
        )

    forward = lines == 4
    inner = lax.rem(line // 2 + line, 2) == 1

    def line_copy(e, h, away=None):
        part = pl.ds(h * cut, cut)
        z = flip(line, e & -e if away is None else away, lines)
        return copy(line_out.at[e, part], line_in.at[e, part], line_sem, (e, h), z, pair, core)

    def mass_copy(peer):
        return pltpu.make_async_remote_copy(
            src_ref=mass_out.at[peer],
            dst_ref=mass_in.at[me],
            send_sem=mass_sem.at[0],
            recv_sem=mass_sem.at[1],
            device_id=(group, peer),
            device_id_type=MESH,
        )

    def partial(*owners):
        size = own * len(owners)
        row = lax.broadcasted_iota(jnp.int32, (size, 1), 0)
        want = row + owners[0] * own
        if len(owners) == 2:
            want = jnp.where(row < own, want, row - own + owners[1] * own)
        here = pl.ds(0, size)
        sums[here, :] = jnp.zeros((size, width), jnp.float32)
        weights[here, :] = jnp.zeros((size, LANES), jnp.float32)

        @pl.loop(0, local // tile)
        def _(t):
            part = pl.ds(pl.multiple_of(t * tile, tile), tile)
            hit = assign_ref[:, part] == want
            value = jnp.where(hit, mass_ref[:, part], 0.0)
            fold = value[:, :LANES]
            for s in range(LANES, tile, LANES):
                fold = fold + value[:, s : s + LANES]
            weights[here, :] += fold
            onehot = jnp.where(hit, 1.0, 0.0).astype(jnp.bfloat16)
            sums[here, :] += jnp.dot(onehot, moved[part, :], preferred_element_type=jnp.float32)

        weight = jnp.sum(weights[here, :], axis=1, keepdims=True)
        flat = jnp.broadcast_to(weight, (size, LANES)).T
        for s, owner in enumerate(owners):
            mass_out[owner] = flat[0:1, s * own : (s + 1) * own]

    def both(e, y):
        z = flip(line, e, lines)
        return at(z, y, 1 - core), at(z, y, core)

    def export(e, q):
        core_out[e, q] = sums[:own, :].astype(jnp.bfloat16)
        core_copy(e, q).start()

    def opening(e):
        theirs, ours = both(e, 1 - pair)
        partial(theirs)
        pl.semaphore_wait(barrier, n - 1)
        export(e, 0)
        mass_copy(theirs).start()
        partial(ours)
        mass_copy(ours).start()
        held[e, 0] = sums[:own, :]

    def compute(e, q):
        theirs, ours = both(e, pair if q else 1 - pair)
        partial(theirs, ours)
        export(e, q)
        mass_copy(theirs).start()
        if e > 0 or q == 0:
            mass_copy(ours).start()
        held[e, q] = sums[own:, :]

    def swap(e):
        core_copy(e, 0).wait_recv()
        for h in range(cuts):
            part = pl.ds(h * cut, cut)
            total = held[e, 0, part, :] + core_in[e, 0, part, :].astype(jnp.float32)
            pair_out[e, part, :] = total.astype(jnp.bfloat16)
            pair_copy(e, h).start()

    def base(e, h):
        if h == 0:
            core_copy(e, 1).wait_recv()
        part = pl.ds(h * cut, cut)
        total = held[e, 1, part, :] + core_in[e, 1, part, :].astype(jnp.float32)
        pair_copy(e, h).wait_recv()
        return total + pair_in[e, part, :].astype(jnp.float32)

    def pass_on(slot, h, away, total):
        line_out[slot, pl.ds(h * cut, cut), :] = total.astype(jnp.bfloat16)
        line_copy(slot, h, away).start()

    def arrived(slot, h):
        line_copy(slot, h, 1).wait_recv()
        return line_in[slot, pl.ds(h * cut, cut), :].astype(jnp.float32)

    def climb_four(e, h):
        part = pl.ds(h * cut, cut)
        if e == 1:

            @pl.when(inner)
            def _():
                pass_on(0, h, 3, held[3, 1, part, :] + arrived(2, h))

        held[e, 1, part, :] = base(e, h)
        if e == 0:
            held[e, 1, part, :] += arrived(1, h)

        @pl.when(inner)
        def _():
            if e == 2:
                pass_on(2, h, 2, held[e, 1, part, :] + arrived(3, h))
            elif e == 1:
                pass_on(1, h, 1, held[e, 1, part, :])
            elif e == 0:
                held[e, 1, part, :] += arrived(0, h)

        @pl.when(jnp.logical_not(inner))
        def _():
            if e > 0:
                pass_on(e, h, 1, held[e, 1, part, :])
            else:
                held[e, 1, part, :] += arrived(2, h)

    def climb(e, h):
        if forward:
            climb_four(e, h)
            return
        part = pl.ds(h * cut, cut)
        total = base(e, h)
        for i in range(steps):
            if e % (2 << i) == 0:
                line_copy(e + (1 << i), h).wait_recv()
                total = total + line_in[e + (1 << i), part, :].astype(jnp.float32)
        if e > 0:
            line_out[e, part, :] = total.astype(jnp.bfloat16)
            line_copy(e, h).start()
        else:
            held[e, 1, part, :] = total

    order = list(range(lines - 1, -1, -1))
    opening(order[0])
    swap(order[0])
    for s, e in enumerate(order):
        if s + 1 < lines:
            compute(order[s + 1], 0)
        if s > 0:
            climb(order[s - 1], 1)
        compute(e, 1)
        if s + 1 < lines:
            swap(order[s + 1])
        climb(e, 0)
    climb(0, 1)

    rest = mass_in.at[pl.ds(1, n - 1)]
    pltpu.make_async_copy(rest, rest, mass_sem.at[1]).wait()
    mass_in[me] = mass_out[me]
    weight = jnp.sum(mass_in[...], axis=0)
    eye = lax.broadcasted_iota(jnp.int32, (own, own), 0) == lax.broadcasted_iota(
        jnp.int32, (own, own), 1
    )
    weight = jnp.sum(jnp.where(eye, weight, 0.0), axis=1, keepdims=True)
    two_ref[...] = (held[0, 1] + PRIOR_TWO * init_ref[...]) / (weight + PRIOR_TWO)

    for e in range(lines):
        core_copy(e, 0).wait_send()
        core_copy(e, 1).wait_send()
        for h in range(cuts):
            pair_copy(e, h).wait_send()
            if forward and e in (0, 3):

                @pl.when(inner if e == 0 else jnp.logical_not(inner))
                def _(e=e, h=h):
                    line_copy(e, h, 1).wait_send()

            elif e > 0:
                line_copy(e, h).wait_send()
    pltpu.make_async_copy(rest, rest, mass_sem.at[0]).wait()


def shards(n, points, centroids, coarse_init, assign):
    rows, width = points.shape
    local = centroids.shape[0]
    own = coarse_init.shape[0]
    count = n * rows
    tile = min(2048, local)
    lines = n // 4
    vmem = pl.BlockSpec(memory_space=pltpu.VMEM)
    anywhere = pl.BlockSpec(memory_space=pl.ANY)
    everyone, lse, logits = pl.pallas_call(
        functools.partial(stats_kernel, n, tile),
        out_shape=(
            jax.ShapeDtypeStruct((count, width), jnp.bfloat16),
            jax.ShapeDtypeStruct((1, count), jnp.float32),
            jax.ShapeDtypeStruct((local, count), jnp.float32),
        ),
        in_specs=[vmem, vmem],
        out_specs=(vmem, vmem, vmem),
        scratch_shapes=[
            pltpu.VMEM((2, count), jnp.float32),
            pltpu.VMEM((n - 1, 2, count), jnp.float32),
            pltpu.SemaphoreType.DMA((lines,)),
            pltpu.SemaphoreType.DMA((lines,)),
            pltpu.SemaphoreType.DMA((2,)),
            pltpu.SemaphoreType.DMA((3,)),
        ],
        compiler_params=pltpu.CompilerParams(
            collective_id=0, has_side_effects=True, vmem_limit_bytes=VMEM_LIMIT
        ),
        name="stats",
    )(points, centroids)
    chunk = min(local, max(LANES, tile * 128 // count))
    level_one, moved, mass = pl.pallas_call(
        functools.partial(update_kernel, chunk),
        out_shape=(
            jax.ShapeDtypeStruct((local, width), jnp.bfloat16),
            jax.ShapeDtypeStruct((local, width), jnp.bfloat16),
            jax.ShapeDtypeStruct((1, local), jnp.float32),
        ),
        in_specs=[vmem, vmem, vmem, vmem],
        out_specs=(anywhere, vmem, vmem),
        scratch_shapes=[
            pltpu.VMEM((local, width), jnp.bfloat16),
            pltpu.SemaphoreType.DMA,
        ],
        compiler_params=pltpu.CompilerParams(vmem_limit_bytes=VMEM_LIMIT),
        name="update",
    )(centroids, logits, everyone, lse)
    level_two = pl.pallas_call(
        functools.partial(coarse_kernel, n),
        out_shape=jax.ShapeDtypeStruct((own, width), jnp.float32),
        in_specs=[vmem, vmem, vmem, vmem],
        out_specs=vmem,
        scratch_shapes=[
            pltpu.VMEM((2 * own, width), jnp.float32),
            pltpu.VMEM((2 * own, LANES), jnp.float32),
            pltpu.VMEM((lines, 2, own, width), jnp.bfloat16),
            pltpu.VMEM((lines, 2, own, width), jnp.bfloat16),
            pltpu.VMEM((lines, own, width), jnp.bfloat16),
            pltpu.VMEM((lines, own, width), jnp.bfloat16),
            pltpu.VMEM((lines, own, width), jnp.bfloat16),
            pltpu.VMEM((lines, own, width), jnp.bfloat16),
            pltpu.VMEM((lines, 2, own, width), jnp.float32),
            pltpu.VMEM((n, 1, own), jnp.float32),
            pltpu.VMEM((n, 1, own), jnp.float32),
            pltpu.SemaphoreType.DMA((2, lines, 2)),
            pltpu.SemaphoreType.DMA((2, lines, 2)),
            pltpu.SemaphoreType.DMA((2, lines, 2)),
            pltpu.SemaphoreType.DMA((2,)),
        ],
        compiler_params=pltpu.CompilerParams(
            collective_id=1, has_side_effects=True, vmem_limit_bytes=VMEM_LIMIT
        ),
        name="coarse",
    )(moved, mass, assign.reshape(1, local), coarse_init)
    return (level_one, level_two)


def solution(mesh):
    return jax.shard_map(
        functools.partial(shards, mesh.shape["cent"]),
        mesh=mesh,
        in_specs=(
            P(("groups", "cent"), None),
            P(("groups", "cent"), None),
            P(("groups", "cent"), None),
            P(("groups", "cent")),
        ),
        out_specs=(P(("groups", "cent"), None), P(("groups", "cent"), None)),
        check_vma=False,
    )
```
